256 devices in a mesh: seq: 64 (over x_hi, z, y), mp: 4 (over x_lo, core).
Axes of the slice: x: 4 (x_hi: 2, x_lo: 2; x = x_hi * 2 + x_lo), y: 4, z: 8, core: 2. Of those that a mesh axis runs over, the one named last changes fastest.
Arguments:
- gate_in: bfloat16 [65536, 1024], P('seq', 'mp'), may hold values from -5 to 5
- value_in: bfloat16 [65536, 1024], P('seq', 'mp'), may hold values from -5 to 5
- out_gate: bfloat16 [65536, 1024], P('seq', 'mp'), may hold values from -10 to 10
- filter_taps: bfloat16 [4096, 1024], P('seq', 'mp'), may hold values from -0.09375 to 0.09375
- skip_gain: float32 [1024], P('mp'), may hold values from -4 to 4
Outputs:
- output: bfloat16 [65536, 1024], P('seq', 'mp')
The draws below stay inside these ranges and needn't reach their ends.
All inputs are finite; a program needn't handle non-finite values.
Results may differ from the reference program's by a relative error of at most 0.009.
Values may be sent and summed in bfloat16 or wider, within the bound.
A program may use at most 64 MiB of HBM per device.

```python
import math
import jax
import jax.numpy as jnp
from jax import lax

C = 1024
K = 4096
TOKENS = 65536


def draw_out_gate(key, part):
    first_key, second_key = jax.random.split(jax.random.fold_in(key, 11), 2)
    position = jnp.arange(C, dtype=jnp.float32) / (C - 1)
    ramp = 0.55 * jnp.power(3.0, position)
    channel_scale = jnp.exp(jax.random.uniform(second_key, (C,), jnp.float32, math.log(0.7), math.log(1.4)))
    base = jnp.clip(jax.random.normal(first_key, (TOKENS, C), jnp.float32), -4.0, 4.0)
    return (base * ramp[None, :] * channel_scale[None, :]).astype(jnp.bfloat16)


def block_scale(key, dims, pieces, smallest, largest):
    def one(dim, parts):
        draws = jax.random.uniform(jax.random.fold_in(jax.random.fold_in(key, 6), dim), (parts,), jnp.float32, smallest / len(pieces), largest / len(pieces))
        return jnp.repeat(jnp.exp(draws), dims[dim] // parts).reshape((-1,) + (1,) * (len(dims) - dim - 1))

    loudness = one(*pieces[0])
    for cut in pieces[1:]:
        loudness = loudness * one(*cut)
    return loudness


def gaussian(stream_key, extent, scale, bound, cuts=(), held_as=jnp.bfloat16):
    loudness = block_scale(stream_key, extent, cuts, -0.22, 0.18) if cuts else 1.0
    entries = jax.random.normal(stream_key, extent, jnp.float32) * scale * loudness
    return jnp.minimum(jnp.maximum(entries, -bound), bound).astype(held_as)


def setup_inputs(seed: int = 0) -> dict:
    keys = jax.random.split(jax.random.key(seed), 6)
    return {
        "gate_in": gaussian(keys[0], (TOKENS, C), 1.0, 5.0, ((0, 64), (1, 4))),
        "value_in": gaussian(keys[1], (TOKENS, C), 1.0, 5.0, ((0, 64), (1, 4))),
        "out_gate": draw_out_gate(jax.random.fold_in(keys[5], 71), 0),
        "filter_taps": gaussian(keys[3], (K, C), K ** -0.5, 0.09375, ((0, 64), (1, 4))),
        "skip_gain": gaussian(keys[4], (C,), 1.0, 4.0, ((0, 4),), jnp.float32),
    }


def convolve_group(signal_kernel):
    signal, kernel = signal_kernel
    length = signal.shape[1]
    size = 1 << (length + kernel.shape[1] - 1).bit_length()
    product = jnp.fft.rfft(signal, size) * jnp.fft.rfft(kernel, size)
    return jnp.fft.irfft(product, size)[:, :length]

def reference(gate_in, value_in, out_gate, filter_taps, skip_gain):
    gated = (gate_in.astype(jnp.float32) * value_in.astype(jnp.float32)).astype(jnp.bfloat16)
    group = 32
    signal = gated.astype(jnp.float32).T.reshape(C // group, group, TOKENS)
    kernel = filter_taps.astype(jnp.float32).T.reshape(C // group, group, K)
    convolved = lax.map(convolve_group, (signal, kernel)).reshape(C, TOKENS).T
    mixed = out_gate.astype(jnp.float32) * (convolved + skip_gain[None, :] * gated.astype(jnp.float32))
    power = lax.optimization_barrier(jnp.mean(mixed * mixed, axis=1, keepdims=True))
    return (mixed / jnp.sqrt(power + 1e-05)).astype(jnp.bfloat16)
```

```python
import jax
import jax.numpy as jnp
from jax import lax
from jax.experimental import pallas as pl
from jax.experimental.pallas import tpu as pltpu
from jax.sharding import PartitionSpec as P

MESH = pl.DeviceIdType.MESH
F32 = jnp.float32
BF16 = jnp.bfloat16

C = 1024
B = 256
N = 64
T = 1024
CH = 256
OWN = CH // N
TAPS = 64
WIN = 128
NWIN = 4096 // WIN
BANDS = 2 * 17 + 1
SIZE = T + 64


def peer(me, o):
    hi = (me // 32 + o // 32) % 2
    z = (me // 4 % 8 + o // 4 % 8) % 8
    y = (me % 4 + o % 4) % 4
    return hi * 32 + z * 4 + y


def put(ref, size, first, count, stride, value):
    for h in range(2):
        ref[pl.ds(h * size + first, count, stride=stride), :] = value[:, 128 * h : 128 * h + 128]


def take(ref, size, first, count, stride=1):
    halves = [ref[pl.ds(h * size + first, count, stride=stride), :] for h in range(2)]
    return jnp.concatenate(halves, axis=1)


def kernel(
    gate, value, out_gate, taps, skip, out,
    send_x, send_t, recv_x, recv_t, stage, og_t, skip_t, win, planes, bands, send_y, recv_y,
    part, recv_p, sx, rx, st, rt, sy, ry, sp, rp,
):
    me = lax.axis_index("seq")
    mp = lax.axis_index("mp")
    barrier = pltpu.get_barrier_semaphore()

    def greet(o, carry):
        pl.semaphore_signal(barrier, inc=1, device_id={"seq": peer(me, o)}, device_id_type=MESH)
        return carry

    lax.fori_loop(1, N, greet, 0)
    for k in range(1, 4):
        pl.semaphore_signal(barrier, inc=1, device_id={"mp": (mp + k) % 4}, device_id_type=MESH)

    wide = jnp.concatenate([taps[...].astype(F32), jnp.zeros((128 - TAPS, CH), F32)], axis=0)
    stage[0:CH, :] = wide.T
    rows = [stage[pl.ds(c, N, stride=OWN), :] for c in range(OWN)]
    pairs = jnp.concatenate(
        [rows[0] + pltpu.roll(rows[1], 64, 1), rows[2] + pltpu.roll(rows[3], 64, 1)], axis=1
    )
    for j in range(N):
        send_t[j] = pairs[j : j + 1]

    for q in range(4):
        at = pl.ds(q * B, B)
        gated = (gate[at, :].astype(F32) * value[at, :].astype(F32)).astype(BF16)
        put(stage, SIZE, q, CH, 4, gated.astype(F32).T)
    for j in range(0, N, 8):
        send_x[pl.ds(j, 8)] = take(stage, SIZE, j * 16, 128).astype(BF16).reshape(8, 16, B)
    for q in range(4):
        put(og_t, T, q, CH, 4, out_gate[pl.ds(q * B, B), :].astype(F32).T)
        skip_t[pl.ds(q, CH, stride=4), :] = jnp.broadcast_to(skip[...], (128, CH)).T

    pl.semaphore_wait(barrier, N - 1 + 3)

    def send(src, dst, ssem, rsem):
        def one(o, carry):
            to = peer(me, o)
            pltpu.make_async_remote_copy(
                src.at[to], dst.at[me], ssem, rsem, device_id={"seq": to}, device_id_type=MESH
            ).start()
            return carry

        lax.fori_loop(1, N, one, 0)

    def waits(src, dst, ssem, rsem):
        return pltpu.make_async_remote_copy(
            src.at[pl.ds(0, N - 1)], dst.at[pl.ds(0, N - 1)], ssem, rsem,
            device_id={"seq": peer(me, 1)}, device_id_type=MESH,
        )

    send(send_t, recv_t, st, rt)
    send(send_x, recv_x, sx, rx)
    recv_t[me] = send_t[me]
    recv_x[me] = send_x[me]

    waits(send_t, recv_t, st, rt).wait_recv()
    lane = lax.broadcasted_iota(jnp.int32, (1, WIN), 1)
    win[...] = jnp.zeros_like(win)
    for j in range(NWIN):
        even, odd = recv_t[2 * j], recv_t[2 * j + 1]
        for c in range(OWN):
            half = slice(c // 2 * 128, c // 2 * 128 + 128)
            e, d = even[:, half], odd[:, half]
            row = jnp.where(lane < 64, e, pltpu.roll(d, 64, 1)) if c % 2 == 0 else (
                jnp.where(lane < 64, pltpu.roll(e, 64, 1), d)
            )
            win[c, pl.ds(j + 1, 1), :] = row
    after = lax.broadcasted_iota(jnp.int32, (WIN, WIN), 1) >= lax.broadcasted_iota(
        jnp.int32, (WIN, WIN), 0
    )
    for c in range(OWN):
        bands[c, pl.ds(0, WIN), :] = jnp.zeros((WIN, WIN), BF16)
        bands[c, pl.ds((BANDS - 1) * WIN, WIN), :] = jnp.zeros((WIN, WIN), BF16)

        def band(v, before, c=c):
            row = jnp.broadcast_to(win[c, pl.ds(v + 1, 1), :], (WIN, WIN))
            rolled = pltpu.roll(row, 0, 1, stride=1, stride_axis=0)
            at = pl.multiple_of((BANDS - 2 - v) * WIN, WIN)
            bands[c, pl.ds(at, WIN), :] = jnp.where(after, rolled, before).astype(BF16)
            return rolled

        lax.fori_loop(0, NWIN + 1, band, jnp.zeros((WIN, WIN), F32))

    waits(send_x, recv_x, sx, rx).wait_recv()
    put(stage, SIZE, 0, 64, 1, jnp.zeros((64, B), F32))
    for j in range(0, N, 8):
        put(stage, SIZE, 64 + j * 16, 128, 1, recv_x[pl.ds(j, 8)].reshape(128, B).astype(F32))
    for c in range(OWN):
        for a in range(16):
            first = 16 * (a // 4) + 4 * c + a % 4
            for late in range(2):
                rows = take(stage, SIZE, first + 64 * late, 16, 64)
                planes[c, pl.ds(256 * late + 16 * a, 16), :] = rows.astype(BF16)

    for c in range(OWN):
        total = jnp.zeros((256, B), F32)
        for d in range(17):
            left = planes[c, pl.ds((16 - d) * 16, 256), :]
            low = bands[c, pl.ds((33 - 2 * d) * WIN, 2 * WIN), :]
            high = bands[c, pl.ds((32 - 2 * d) * WIN, 2 * WIN), :]
            total += jnp.dot(
                left, jnp.concatenate([low, high], axis=1), preferred_element_type=F32
            )
        for a in range(16):
            first = 16 * (a // 4) + 4 * c + a % 4
            put(stage, SIZE, first, 16, 64, total[16 * a : 16 * a + 16])
    for j in range(0, N, 8):
        send_y[pl.ds(j, 8)] = take(stage, SIZE, j * 16, 128).astype(BF16).reshape(8, 16, B)
    recv_y[me] = send_y[me]
    send(send_y, recv_y, sy, ry)
    waits(send_y, recv_y, sy, ry).wait_recv()

    squares = jnp.zeros((8, B), F32)
    for j in range(0, N, 2):
        at = pl.ds(j * 16, 32)
        gain = skip_t[at, :]
        conv = recv_y[pl.ds(j, 2)].reshape(32, B).astype(F32)
        gated = send_x[pl.ds(j, 2)].reshape(32, B).astype(F32)
        mixed = take(og_t, T, j * 16, 32) * (conv + jnp.concatenate([gain, gain], axis=1) * gated)
        put(stage, SIZE, j * 16, 32, 1, mixed)
        squares += jnp.sum((mixed * mixed).reshape(4, 8, B), axis=0)
    part[0:4, :] = squares[0:4] + squares[4:8]
    part[4:8, :] = jnp.zeros((4, B), F32)
    copies = []
    for k in range(1, 4):
        copy = pltpu.make_async_remote_copy(
            part, recv_p.at[k - 1], sp.at[k - 1], rp.at[k - 1],
            device_id={"mp": (mp + k) % 4}, device_id_type=MESH,
        )
        copy.start()
        copies.append(copy)
    power = part[0:4, :]
    for copy in copies:
        copy.wait_recv()
    power = power + recv_p[0][0:4] + recv_p[1][0:4] + recv_p[2][0:4]
    scale = 1.0 / jnp.sqrt(power / C + 1e-05)
    for q in range(4):
        mixed = take(stage, SIZE, q, CH, 4) * scale[q : q + 1]
        out[pl.ds(q * B, B), :] = mixed.T.astype(BF16)
    for copy in copies:
        copy.wait_send()
    waits(send_t, recv_t, st, rt).wait_send()
    waits(send_x, recv_x, sx, rx).wait_send()
    waits(send_y, recv_y, sy, ry).wait_send()


def local(gate_in, value_in, out_gate, filter_taps, skip_gain):
    vmem = pl.BlockSpec(memory_space=pltpu.VMEM)
    dma = pltpu.SemaphoreType.DMA
    return pl.pallas_call(
        kernel,
        out_shape=jax.ShapeDtypeStruct((T, CH), BF16),
        in_specs=[vmem] * 5,
        out_specs=vmem,
        scratch_shapes=[
            pltpu.VMEM((N, 16, B), BF16),
            pltpu.VMEM((N, 1, B), F32),
            pltpu.VMEM((N, 16, B), BF16),
            pltpu.VMEM((N, 1, B), F32),
            pltpu.VMEM((2 * SIZE, 128), F32),
            pltpu.VMEM((2 * T, 128), F32),
            pltpu.VMEM((T, 128), F32),
            pltpu.VMEM((OWN, 40, WIN), F32),
            pltpu.VMEM((OWN, 512, B), BF16),
            pltpu.VMEM((OWN, BANDS * WIN, WIN), BF16),
            pltpu.VMEM((N, 16, B), BF16),
            pltpu.VMEM((N, 16, B), BF16),
            pltpu.VMEM((8, B), F32),
            pltpu.VMEM((3, 8, B), F32),
            dma, dma, dma, dma, dma, dma, dma((3,)), dma((3,)),
        ],
        compiler_params=pltpu.CompilerParams(
            collective_id=0, has_side_effects=True, vmem_limit_bytes=48 * 2**20
        ),
    )(gate_in, value_in, out_gate, filter_taps, skip_gain.reshape(1, CH))


def solution(mesh):
    return jax.shard_map(
        local,
        mesh=mesh,
        in_specs=(P("seq", "mp"), P("seq", "mp"), P("seq", "mp"), P("seq", "mp"), P("mp")),
        out_specs=P("seq", "mp"),
        check_vma=False,
    )
```

```python
import jax
import jax.numpy as jnp
from jax import lax
from jax.experimental import pallas as pl
from jax.experimental.pallas import tpu as pltpu
from jax.sharding import PartitionSpec as P

MESH = pl.DeviceIdType.MESH
F32 = jnp.float32
BF16 = jnp.bfloat16

C = 1024
B = 256
N = 64
T = 1024
CH = 256
OWN = CH // N
TAPS = 64
WIN = 128
NWIN = 4096 // WIN
BANDS = 2 * 17 + 1
SIZE = T + 64


def peer(me, o):
    hi = (me // 32 + o // 32) % 2
    z = (me // 4 % 8 + o // 4 % 8) % 8
    y = (me % 4 + o % 4) % 4
    return hi * 32 + z * 4 + y


def put(ref, size, first, count, stride, value):
    for h in range(2):
        ref[pl.ds(h * size + first, count, stride=stride), :] = value[:, 128 * h : 128 * h + 128]


def take(ref, size, first, count, stride=1):
    halves = [ref[pl.ds(h * size + first, count, stride=stride), :] for h in range(2)]
    return jnp.concatenate(halves, axis=1)


def kernel(
    gate_h, value_h, out_gate_h, taps_h, skip_h, out,
    gate, value, out_gate, taps, skip,
    send_x, send_t, recv_x, recv_t, stage, og_t, skip_t, win, planes, bands, send_y, recv_y,
    part, recv_p, loaded, sx, rx, st, rt, sy, ry, sp, rp,
):
    me = lax.axis_index("seq")
    mp = lax.axis_index("mp")
    barrier = pltpu.get_barrier_semaphore()

    def greet(o, carry):
        pl.semaphore_signal(barrier, inc=1, device_id={"seq": peer(me, o)}, device_id_type=MESH)
        return carry

    lax.fori_loop(1, N, greet, 0)
    for k in range(1, 4):
        pl.semaphore_signal(barrier, inc=1, device_id={"mp": (mp + k) % 4}, device_id_type=MESH)

    pairs = ((taps_h, taps), (gate_h, gate), (value_h, value), (out_gate_h, out_gate), (skip_h, skip))
    loads = [pltpu.make_async_copy(a, b, loaded.at[i]) for i, (a, b) in enumerate(pairs)]
    for load in loads:
        load.start()

    loads[0].wait()
    wide = jnp.concatenate([taps[...].astype(F32), jnp.zeros((128 - TAPS, CH), F32)], axis=0)
    stage[0:CH, :] = wide.T
    rows = [stage[pl.ds(c, N, stride=OWN), :] for c in range(OWN)]
    pairs = jnp.concatenate(
        [rows[0] + pltpu.roll(rows[1], 64, 1), rows[2] + pltpu.roll(rows[3], 64, 1)], axis=1
    )
    for j in range(N):
        send_t[j] = pairs[j : j + 1]

    loads[1].wait()
    loads[2].wait()
    for q in range(4):
        at = pl.ds(q * B, B)
        gated = (gate[at, :].astype(F32) * value[at, :].astype(F32)).astype(BF16)
        put(stage, SIZE, q, CH, 4, gated.astype(F32).T)
    for j in range(0, N, 8):
        send_x[pl.ds(j, 8)] = take(stage, SIZE, j * 16, 128).astype(BF16).reshape(8, 16, B)
    pl.semaphore_wait(barrier, N - 1 + 3)

    def send(src, dst, ssem, rsem):
        def one(o, carry):
            to = peer(me, o)
            pltpu.make_async_remote_copy(
                src.at[to], dst.at[me], ssem, rsem, device_id={"seq": to}, device_id_type=MESH
            ).start()
            return carry

        lax.fori_loop(1, N, one, 0)

    def waits(src, dst, ssem, rsem):
        return pltpu.make_async_remote_copy(
            src.at[pl.ds(0, N - 1)], dst.at[pl.ds(0, N - 1)], ssem, rsem,
            device_id={"seq": peer(me, 1)}, device_id_type=MESH,
        )

    send(send_t, recv_t, st, rt)
    send(send_x, recv_x, sx, rx)
    recv_t[me] = send_t[me]
    recv_x[me] = send_x[me]

    loads[3].wait()
    loads[4].wait()
    for q in range(4):
        put(og_t, T, q, CH, 4, out_gate[pl.ds(q * B, B), :].astype(F32).T)
        skip_t[pl.ds(q, CH, stride=4), :] = jnp.broadcast_to(skip[...], (128, CH)).T

    waits(send_t, recv_t, st, rt).wait_recv()
    lane = lax.broadcasted_iota(jnp.int32, (1, WIN), 1)
    win[...] = jnp.zeros_like(win)
    for j in range(NWIN):
        even, odd = recv_t[2 * j], recv_t[2 * j + 1]
        for c in range(OWN):
            half = slice(c // 2 * 128, c // 2 * 128 + 128)
            e, d = even[:, half], odd[:, half]
            row = jnp.where(lane < 64, e, pltpu.roll(d, 64, 1)) if c % 2 == 0 else (
                jnp.where(lane < 64, pltpu.roll(e, 64, 1), d)
            )
            win[c, pl.ds(j + 1, 1), :] = row
    after = lax.broadcasted_iota(jnp.int32, (WIN, WIN), 1) >= lax.broadcasted_iota(
        jnp.int32, (WIN, WIN), 0
    )
    def banded(c, carry):
        before = jnp.zeros((WIN, WIN), F32)
        bands[c, pl.ds((BANDS - 1) * WIN, WIN), :] = before.astype(BF16)
        for v in range(NWIN + 1):
            row = jnp.broadcast_to(win[c, v + 1 : v + 2, :], (WIN, WIN))
            rolled = pltpu.roll(row, 0, 1, stride=1, stride_axis=0)
            at = pl.ds((BANDS - 2 - v) * WIN, WIN)
            bands[c, at, :] = jnp.where(after, rolled, before).astype(BF16)
            before = rolled
        bands[c, pl.ds(0, WIN), :] = jnp.zeros((WIN, WIN), BF16)
        return carry

    lax.fori_loop(0, OWN, banded, 0)

    waits(send_x, recv_x, sx, rx).wait_recv()
    put(stage, SIZE, 0, 64, 1, jnp.zeros((64, B), F32))
    for j in range(0, N, 8):
        put(stage, SIZE, 64 + j * 16, 128, 1, recv_x[pl.ds(j, 8)].reshape(128, B).astype(F32))
    for c in range(OWN):
        for a in range(16):
            first = 16 * (a // 4) + 4 * c + a % 4
            for late in range(2):
                rows = take(stage, SIZE, first + 64 * late, 16, 64)
                planes[c, pl.ds(256 * late + 16 * a, 16), :] = rows.astype(BF16)

    for c in range(OWN):
        total = jnp.zeros((256, B), F32)
        for d in range(17):
            left = planes[c, pl.ds((16 - d) * 16, 256), :]
            low = bands[c, pl.ds((33 - 2 * d) * WIN, 2 * WIN), :]
            high = bands[c, pl.ds((32 - 2 * d) * WIN, 2 * WIN), :]
            total += jnp.dot(
                left, jnp.concatenate([low, high], axis=1), preferred_element_type=F32
            )
        for a in range(16):
            first = 16 * (a // 4) + 4 * c + a % 4
            put(stage, SIZE, first, 16, 64, total[16 * a : 16 * a + 16])
    for j in range(0, N, 8):
        send_y[pl.ds(j, 8)] = take(stage, SIZE, j * 16, 128).astype(BF16).reshape(8, 16, B)
    recv_y[me] = send_y[me]
    send(send_y, recv_y, sy, ry)
    waits(send_y, recv_y, sy, ry).wait_recv()

    squares = jnp.zeros((8, B), F32)
    for j in range(0, N, 2):
        at = pl.ds(j * 16, 32)
        gain = skip_t[at, :]
        conv = recv_y[pl.ds(j, 2)].reshape(32, B).astype(F32)
        gated = send_x[pl.ds(j, 2)].reshape(32, B).astype(F32)
        mixed = take(og_t, T, j * 16, 32) * (conv + jnp.concatenate([gain, gain], axis=1) * gated)
        put(stage, SIZE, j * 16, 32, 1, mixed)
        squares += jnp.sum((mixed * mixed).reshape(4, 8, B), axis=0)
    part[0:4, :] = squares[0:4] + squares[4:8]
    part[4:8, :] = jnp.zeros((4, B), F32)
    copies = []
    for k in range(1, 4):
        copy = pltpu.make_async_remote_copy(
            part, recv_p.at[k - 1], sp.at[k - 1], rp.at[k - 1],
            device_id={"mp": (mp + k) % 4}, device_id_type=MESH,
        )
        copy.start()
        copies.append(copy)
    power = part[0:4, :]
    for copy in copies:
        copy.wait_recv()
    power = power + recv_p[0][0:4] + recv_p[1][0:4] + recv_p[2][0:4]
    scale = 1.0 / jnp.sqrt(power / C + 1e-05)
    for q in range(4):
        mixed = take(stage, SIZE, q, CH, 4) * scale[q : q + 1]
        out[pl.ds(q * B, B), :] = mixed.T.astype(BF16)
    for copy in copies:
        copy.wait_send()
    waits(send_t, recv_t, st, rt).wait_send()
    waits(send_x, recv_x, sx, rx).wait_send()
    waits(send_y, recv_y, sy, ry).wait_send()


def local(gate_in, value_in, out_gate, filter_taps, skip_gain):
    vmem = pl.BlockSpec(memory_space=pltpu.VMEM)
    dma = pltpu.SemaphoreType.DMA
    return pl.pallas_call(
        kernel,
        out_shape=jax.ShapeDtypeStruct((T, CH), BF16),
        in_specs=[pl.BlockSpec(memory_space=pltpu.HBM)] * 5,
        out_specs=vmem,
        scratch_shapes=[
            pltpu.VMEM((T, CH), BF16),
            pltpu.VMEM((T, CH), BF16),
            pltpu.VMEM((T, CH), BF16),
            pltpu.VMEM((TAPS, CH), BF16),
            pltpu.VMEM((1, CH), F32),
            pltpu.VMEM((N, 16, B), BF16),
            pltpu.VMEM((N, 1, B), F32),
            pltpu.VMEM((N, 16, B), BF16),
            pltpu.VMEM((N, 1, B), F32),
            pltpu.VMEM((2 * SIZE, 128), F32),
            pltpu.VMEM((2 * T, 128), F32),
            pltpu.VMEM((T, 128), F32),
            pltpu.VMEM((OWN, 40, WIN), F32),
            pltpu.VMEM((OWN, 512, B), BF16),
            pltpu.VMEM((OWN, BANDS * WIN, WIN), BF16),
            pltpu.VMEM((N, 16, B), BF16),
            pltpu.VMEM((N, 16, B), BF16),
            pltpu.VMEM((8, B), F32),
            pltpu.VMEM((3, 8, B), F32),
            dma((5,)), dma, dma, dma, dma, dma, dma, dma((3,)), dma((3,)),
        ],
        compiler_params=pltpu.CompilerParams(
            collective_id=0, has_side_effects=True, vmem_limit_bytes=48 * 2**20
        ),
    )(gate_in, value_in, out_gate, filter_taps, skip_gain.reshape(1, CH))


def solution(mesh):
    return jax.shard_map(
        local,
        mesh=mesh,
        in_specs=(P("seq", "mp"), P("seq", "mp"), P("seq", "mp"), P("seq", "mp"), P("mp")),
        out_specs=P("seq", "mp"),
        check_vma=False,
    )
```

```python
import jax
import jax.numpy as jnp
from jax import lax
from jax.experimental import pallas as pl
from jax.experimental.pallas import tpu as pltpu
from jax.sharding import PartitionSpec as P

MESH = pl.DeviceIdType.MESH
F32 = jnp.float32
BF16 = jnp.bfloat16

C = 1024
B = 256
N = 64
T = 1024
CH = 256
OWN = CH // N
TAPS = 64
WIN = 128
NWIN = 4096 // WIN
BANDS = 2 * 17 + 1
GROUPS = 2
PER = OWN // GROUPS
ROWS = 4 * PER
WORK = (N + 4) * ROWS


def peer(me, o):
    hi = (me // 32 + o // 32) % 2
    z = (me // 4 % 8 + o // 4 % 8) % 8
    y = (me % 4 + o % 4) % 4
    return hi * 32 + z * 4 + y


def put(ref, size, first, count, stride, value):
    for h in range(2):
        ref[pl.ds(h * size + first, count, stride=stride), :] = value[:, 128 * h : 128 * h + 128]


def take(ref, size, first, count, stride=1):
    halves = [ref[pl.ds(h * size + first, count, stride=stride), :] for h in range(2)]
    return jnp.concatenate(halves, axis=1)


def kernel(
    gate_h, value_h, out_gate_h, taps_h, skip_h, out,
    gate, value, out_gate, taps, skip,
    send_x, send_t, recv_x, recv_t, stage, work, turned, og_t, skip_t, win, planes, bands, send_y, recv_y,
    part, recv_p, loaded, sx, rx, st, rt, sy, ry, sp, rp,
):
    me = lax.axis_index("seq")
    mp = lax.axis_index("mp")
    barrier = pltpu.get_barrier_semaphore()

    def greet(o, carry):
        pl.semaphore_signal(barrier, inc=1, device_id={"seq": peer(me, o)}, device_id_type=MESH)
        return carry

    lax.fori_loop(1, N, greet, 0)
    for k in range(1, 4):
        pl.semaphore_signal(barrier, inc=1, device_id={"mp": (mp + k) % 4}, device_id_type=MESH)

    pairs = ((taps_h, taps), (gate_h, gate), (value_h, value), (out_gate_h, out_gate), (skip_h, skip))
    loads = [pltpu.make_async_copy(a, b, loaded.at[i]) for i, (a, b) in enumerate(pairs)]
    for load in loads:
        load.start()

    loads[0].wait()
    wide = jnp.concatenate([taps[...].astype(F32), jnp.zeros((128 - TAPS, CH), F32)], axis=0)
    stage[0:CH, :] = wide.T
    rows = [stage[pl.ds(c, N, stride=OWN), :] for c in range(OWN)]
    pairs = jnp.concatenate(
        [rows[0] + pltpu.roll(rows[1], 64, 1), rows[2] + pltpu.roll(rows[3], 64, 1)], axis=1
    )
    for j in range(N):
        send_t[j] = pairs[j : j + 1]

    loads[1].wait()
    loads[2].wait()
    for q in range(4):
        at = pl.ds(q * B, B)
        gated = (gate[at, :].astype(F32) * value[at, :].astype(F32)).astype(BF16)
        put(stage, T, q, CH, 4, gated.astype(F32).T)
    for j in range(0, N, 8):
        block = take(stage, T, j * 16, 128).reshape(8, GROUPS, ROWS, B).astype(BF16)
        for g in range(GROUPS):
            send_x[g, pl.ds(j, 8)] = block[:, g]
    pl.semaphore_wait(barrier, N - 1 + 3)

    def send(src, dst, ssem, rsem):
        def one(o, carry):
            to = peer(me, o)
            pltpu.make_async_remote_copy(
                src.at[to], dst.at[me], ssem, rsem, device_id={"seq": to}, device_id_type=MESH
            ).start()
            return carry

        lax.fori_loop(1, N, one, 0)

    def waits(src, dst, ssem, rsem):
        return pltpu.make_async_remote_copy(
            src.at[pl.ds(0, N - 1)], dst.at[pl.ds(0, N - 1)], ssem, rsem,
            device_id={"seq": peer(me, 1)}, device_id_type=MESH,
        )

    send(send_t, recv_t, st, rt)
    for g in range(GROUPS):
        send(send_x.at[g], recv_x.at[g], sx.at[g], rx.at[g])
    recv_t[me] = send_t[me]
    for g in range(GROUPS):
        recv_x[g, me] = send_x[g, me]

    loads[3].wait()
    loads[4].wait()
    for q in range(4):
        put(og_t, T, q, CH, 4, out_gate[pl.ds(q * B, B), :].astype(F32).T)
        skip_t[pl.ds(q, CH, stride=4), :] = jnp.broadcast_to(skip[...], (128, CH)).T

    waits(send_t, recv_t, st, rt).wait_recv()
    lane = lax.broadcasted_iota(jnp.int32, (1, WIN), 1)
    win[...] = jnp.zeros_like(win)
    for j in range(NWIN):
        even, odd = recv_t[2 * j], recv_t[2 * j + 1]
        for c in range(OWN):
            half = slice(c // 2 * 128, c // 2 * 128 + 128)
            e, d = even[:, half], odd[:, half]
            row = jnp.where(lane < 64, e, pltpu.roll(d, 64, 1)) if c % 2 == 0 else (
                jnp.where(lane < 64, pltpu.roll(e, 64, 1), d)
            )
            win[c, pl.ds(j + 1, 1), :] = row
    after = lax.broadcasted_iota(jnp.int32, (WIN, WIN), 1) >= lax.broadcasted_iota(
        jnp.int32, (WIN, WIN), 0
    )

    def banded(c, carry):
        before = jnp.zeros((WIN, WIN), F32)
        bands[c, pl.ds((BANDS - 1) * WIN, WIN), :] = before.astype(BF16)
        for v in range(NWIN + 1):
            row = jnp.broadcast_to(win[c, v + 1 : v + 2, :], (WIN, WIN))
            rolled = pltpu.roll(row, 0, 1, stride=1, stride_axis=0)
            at = pl.ds((BANDS - 2 - v) * WIN, WIN)
            bands[c, at, :] = jnp.where(after, rolled, before).astype(BF16)
            before = rolled
        bands[c, pl.ds(0, WIN), :] = jnp.zeros((WIN, WIN), BF16)
        return carry

    lax.fori_loop(0, OWN, banded, 0)

    put(work, WORK, 0, 4 * ROWS, 1, jnp.zeros((4 * ROWS, B), F32))
    for g in range(GROUPS):
        waits(send_x.at[g], recv_x.at[g], sx.at[g], rx.at[g]).wait_recv()
        for j in range(0, N, 8):
            block = recv_x[g, pl.ds(j, 8)].reshape(8 * ROWS, B).astype(F32)
            put(work, WORK, (4 + j) * ROWS, 8 * ROWS, 1, block)
        for c in range(PER):
            for a in range(16):
                first = ROWS * (a // 4) + 4 * c + a % 4
                for late in range(2):
                    rows = take(work, WORK, first + 4 * ROWS * late, 16, 4 * ROWS)
                    planes[c, pl.ds(256 * late + 16 * a, 16), :] = rows.astype(BF16)
        for c in range(PER):
            total = jnp.zeros((256, B), F32)
            for d in range(17):
                left = planes[c, pl.ds((16 - d) * 16, 256), :]
                low = bands[PER * g + c, pl.ds((33 - 2 * d) * WIN, 2 * WIN), :]
                high = bands[PER * g + c, pl.ds((32 - 2 * d) * WIN, 2 * WIN), :]
                total += jnp.dot(
                    left, jnp.concatenate([low, high], axis=1), preferred_element_type=F32
                )
            for a in range(16):
                first = ROWS * (4 + a // 4) + 4 * c + a % 4
                put(work, WORK, first, 16, 4 * ROWS, total[16 * a : 16 * a + 16])
        for j in range(0, N, 8):
            block = take(work, WORK, (4 + j) * ROWS, 8 * ROWS).astype(BF16)
            send_y[g, pl.ds(j, 8)] = block.reshape(8, ROWS, B)
        recv_y[g, me] = send_y[g, me]
        send(send_y.at[g], recv_y.at[g], sy.at[g], ry.at[g])

    squares = jnp.zeros((8, B), F32)
    for g in range(GROUPS):
        waits(send_y.at[g], recv_y.at[g], sy.at[g], ry.at[g]).wait_recv()
        for j in range(N):
            at = pl.ds(j * 16 + g * ROWS, ROWS)
            gain = skip_t[at, :]
            gated = send_x[g, j].astype(F32)
            mixed = take(og_t, T, j * 16 + g * ROWS, ROWS) * (
                recv_y[g, j].astype(F32) + jnp.concatenate([gain, gain], axis=1) * gated
            )
            put(stage, T, j * 16 + g * ROWS, ROWS, 1, mixed)
            squares += jnp.sum((mixed * mixed).reshape(ROWS // 8, 8, B), axis=0)
    part[0:4, :] = squares[0:4] + squares[4:8]
    part[4:8, :] = jnp.zeros((4, B), F32)
    copies = []
    for k in range(1, 4):
        copy = pltpu.make_async_remote_copy(
            part, recv_p.at[k - 1], sp.at[k - 1], rp.at[k - 1],
            device_id={"mp": (mp + k) % 4}, device_id_type=MESH,
        )
        copy.start()
        copies.append(copy)
    for q in range(4):
        turned[pl.ds(q * B, B), :] = take(stage, T, q, CH, 4).T
    waits(send_t, recv_t, st, rt).wait_send()
    for g in range(GROUPS):
        waits(send_x.at[g], recv_x.at[g], sx.at[g], rx.at[g]).wait_send()
        waits(send_y.at[g], recv_y.at[g], sy.at[g], ry.at[g]).wait_send()
    power = part[0:4, :]
    for copy in copies:
        copy.wait_recv()
    power = power + recv_p[0][0:4] + recv_p[1][0:4] + recv_p[2][0:4]
    scale = 1.0 / jnp.sqrt(power / C + 1e-05)
    for q in range(4):
        column = jnp.broadcast_to(scale[q : q + 1], (128, B)).T
        column = jnp.concatenate([column, column], axis=1)
        out[pl.ds(q * B, B), :] = (turned[pl.ds(q * B, B), :] * column).astype(BF16)
    for copy in copies:
        copy.wait_send()


def local(gate_in, value_in, out_gate, filter_taps, skip_gain):
    vmem = pl.BlockSpec(memory_space=pltpu.VMEM)
    dma = pltpu.SemaphoreType.DMA
    return pl.pallas_call(
        kernel,
        out_shape=jax.ShapeDtypeStruct((T, CH), BF16),
        in_specs=[pl.BlockSpec(memory_space=pltpu.HBM)] * 5,
        out_specs=vmem,
        scratch_shapes=[
            pltpu.VMEM((T, CH), BF16),
            pltpu.VMEM((T, CH), BF16),
            pltpu.VMEM((T, CH), BF16),
            pltpu.VMEM((TAPS, CH), BF16),
            pltpu.VMEM((1, CH), F32),
            pltpu.VMEM((GROUPS, N, ROWS, B), BF16),
            pltpu.VMEM((N, 1, B), F32),
            pltpu.VMEM((GROUPS, N, ROWS, B), BF16),
            pltpu.VMEM((N, 1, B), F32),
            pltpu.VMEM((2 * T, 128), F32),
            pltpu.VMEM((2 * WORK, 128), F32),
            pltpu.VMEM((T, CH), F32),
            pltpu.VMEM((2 * T, 128), F32),
            pltpu.VMEM((T, 128), F32),
            pltpu.VMEM((OWN, 40, WIN), F32),
            pltpu.VMEM((PER, 512, B), BF16),
            pltpu.VMEM((OWN, BANDS * WIN, WIN), BF16),
            pltpu.VMEM((GROUPS, N, ROWS, B), BF16),
            pltpu.VMEM((GROUPS, N, ROWS, B), BF16),
            pltpu.VMEM((8, B), F32),
            pltpu.VMEM((3, 8, B), F32),
            dma((5,)), dma((GROUPS,)), dma((GROUPS,)), dma, dma, dma((GROUPS,)), dma((GROUPS,)),
            dma((3,)), dma((3,)),
        ],
        compiler_params=pltpu.CompilerParams(
            collective_id=0, has_side_effects=True, vmem_limit_bytes=67043328
        ),
    )(gate_in, value_in, out_gate, filter_taps, skip_gain.reshape(1, CH))


def solution(mesh):
    return jax.shard_map(
        local,
        mesh=mesh,
        in_specs=(P("seq", "mp"), P("seq", "mp"), P("seq", "mp"), P("seq", "mp"), P("mp")),
        out_specs=P("seq", "mp"),
        check_vma=False,
    )
```

```python
import jax
import jax.numpy as jnp
from jax import lax
from jax.experimental import pallas as pl
from jax.experimental.pallas import tpu as pltpu
from jax.sharding import PartitionSpec as P

MESH = pl.DeviceIdType.MESH
F32 = jnp.float32
BF16 = jnp.bfloat16

C = 1024
B = 256
N = 64
T = 1024
CH = 256
TAPS = 64
WIN = 128
NWIN = 4096 // WIN
BANDS = 2 * 17 + 1
PER = 2
PAIRS = CH // PER
ROWS = 4 * PER
WORK = (N + 4) * ROWS
OWN = PAIRS // N


def place(me):
    return me // 32, me // 4 % 8, me % 4


ALONG = (4, 3, 5, 2, 6, 1, 7, 0)


def put(ref, size, first, count, stride, value):
    for h in range(2):
        ref[pl.ds(h * size + first, count, stride=stride), :] = value[:, 128 * h : 128 * h + 128]


def take(ref, size, first, count, stride=1):
    halves = [ref[pl.ds(h * size + first, count, stride=stride), :] for h in range(2)]
    return jnp.concatenate(halves, axis=1)


def kernel(
    gate_h, value_h, out_gate_h, taps_h, skip_h, out,
    gate, value, out_gate, taps, skip,
    send_x, send_t, recv_x, recv_t, stage, work, turned, og_t, skip_t, win, planes, bands, send_y, recv_y,
    part, recv_p, loaded, sx, rx, st, rt, sy, ry, sp, rp,
):
    me = lax.axis_index("seq")
    mp = lax.axis_index("mp")
    barrier = pltpu.get_barrier_semaphore()

    x, z, y = place(me)
    along = [(z + dz) % 8 * 4 for dz in ALONG]

    def others(visit):
        def column(r, last):
            dx, dy = (r + 1) % 8 // 4, (r + 1) % 4
            base = (x + dx) % 2 * 32 + (y + dy) % 4
            for plane in along[: 8 - last]:
                visit(base + plane)

        def each(r, carry):
            column(r, 0)
            return carry

        lax.fori_loop(0, 7, each, 0)
        column(7, 1)

    others(
        lambda to: pl.semaphore_signal(
            barrier, inc=1, device_id={"seq": to}, device_id_type=MESH
        )
    )
    for k in range(1, 4):
        pl.semaphore_signal(barrier, inc=1, device_id={"mp": (mp + k) % 4}, device_id_type=MESH)

    pairs = ((taps_h, taps), (gate_h, gate), (value_h, value), (out_gate_h, out_gate), (skip_h, skip))
    loads = [pltpu.make_async_copy(a, b, loaded.at[i]) for i, (a, b) in enumerate(pairs)]
    for load in loads:
        load.start()

    loads[0].wait()
    wide = jnp.concatenate([taps[...].astype(F32), jnp.zeros((128 - TAPS, CH), F32)], axis=0)
    stage[0:CH, :] = wide.T
    first, second = (stage[pl.ds(c, PAIRS, stride=PER), :] for c in range(PER))
    both = first + pltpu.roll(second, 64, 1)
    for j in range(PAIRS):
        send_t[j] = both[j : j + 1]

    loads[1].wait()
    loads[2].wait()
    for q in range(4):
        at = pl.ds(q * B, B)
        gated = (gate[at, :].astype(F32) * value[at, :].astype(F32)).astype(BF16)
        put(stage, T, q, CH, 4, gated.astype(F32).T)
    for j in range(0, N, 8):
        block = take(stage, T, j * 16, 128).astype(BF16)
        send_x[pl.ds(2 * j, 16)] = block.reshape(16, ROWS, B)
    pl.semaphore_wait(barrier, N - 1 + 3)

    def send(src, dst, ssem, rsem, to):
        pltpu.make_async_remote_copy(
            src, dst, ssem, rsem, device_id={"seq": to}, device_id_type=MESH
        ).start()

    def forth_taps(to):
        send(send_t.at[pl.ds(OWN * to, OWN)], recv_t.at[pl.ds(OWN * me, OWN)], st, rt, to)

    def forth(g):
        others(
            lambda to: send(
                send_x.at[OWN * to + g], recv_x.at[g, me], sx.at[g], rx.at[g], to
            )
        )

    def back(g):
        others(
            lambda to: send(
                send_y.at[g, to], recv_y.at[OWN * me + g], sy.at[g], ry.at[g], to
            )
        )

    def of_slabs(ref, n, ssem, rsem):
        return pltpu.make_async_remote_copy(
            ref.at[pl.ds(0, n)], ref.at[pl.ds(0, n)], ssem, rsem,
            device_id={"seq": (me + 1) % N}, device_id_type=MESH,
        )

    others(forth_taps)
    for g in range(OWN):
        forth(g)
    for g in range(OWN):
        recv_t[OWN * me + g] = send_t[OWN * me + g]
        recv_x[g, me] = send_x[OWN * me + g]

    loads[3].wait()
    loads[4].wait()
    for q in range(4):
        put(og_t, T, q, CH, 4, out_gate[pl.ds(q * B, B), :].astype(F32).T)
        skip_t[pl.ds(q, CH, stride=4), :] = jnp.broadcast_to(skip[...], (128, CH)).T

    lane = lax.broadcasted_iota(jnp.int32, (1, WIN), 1)
    win[...] = jnp.zeros_like(win)
    of_slabs(recv_t, OWN * (N - 1), st, rt).wait_recv()
    for g in range(OWN):
        for j in range(NWIN):
            even, odd = recv_t[2 * OWN * j + g], recv_t[OWN * (2 * j + 1) + g]
            win[2 * g, pl.ds(j + 1, 1), :] = jnp.where(lane < 64, even, pltpu.roll(odd, 64, 1))
            win[2 * g + 1, pl.ds(j + 1, 1), :] = jnp.where(lane < 64, pltpu.roll(even, 64, 1), odd)
    after = lax.broadcasted_iota(jnp.int32, (WIN, WIN), 1) >= lax.broadcasted_iota(
        jnp.int32, (WIN, WIN), 0
    )

    def banded(c, carry):
        before = jnp.zeros((WIN, WIN), F32)
        bands[c, pl.ds((BANDS - 1) * WIN, WIN), :] = before.astype(BF16)
        for v in range(NWIN + 1):
            row = jnp.broadcast_to(win[c, v + 1 : v + 2, :], (WIN, WIN))
            rolled = pltpu.roll(row, 0, 1, stride=1, stride_axis=0)
            at = pl.ds((BANDS - 2 - v) * WIN, WIN)
            bands[c, at, :] = jnp.where(after, rolled, before).astype(BF16)
            before = rolled
        bands[c, pl.ds(0, WIN), :] = jnp.zeros((WIN, WIN), BF16)
        return carry

    lax.fori_loop(0, PER * OWN, banded, 0)

    put(work, WORK, 0, 4 * ROWS, 1, jnp.zeros((4 * ROWS, B), F32))

    def convolve(g):
        of_slabs(recv_x.at[g], N - 1, sx.at[g], rx.at[g]).wait_recv()
        for j in range(0, N, 8):
            block = recv_x[g, pl.ds(j, 8)].reshape(8 * ROWS, B).astype(F32)
            put(work, WORK, (4 + j) * ROWS, 8 * ROWS, 1, block)
        for c in range(PER):
            for a in range(16):
                first = ROWS * (a // 4) + 4 * c + a % 4
                for late in range(2):
                    rows = take(work, WORK, first + 4 * ROWS * late, 16, 4 * ROWS)
                    planes[c, pl.ds(256 * late + 16 * a, 16), :] = rows.astype(BF16)
        for c in range(PER):
            total = jnp.zeros((256, B), F32)
            for d in range(17):
                left = planes[c, pl.ds((16 - d) * 16, 256), :]
                low = bands[PER * g + c, pl.ds((33 - 2 * d) * WIN, 2 * WIN), :]
                high = bands[PER * g + c, pl.ds((32 - 2 * d) * WIN, 2 * WIN), :]
                total += jnp.dot(
                    left, jnp.concatenate([low, high], axis=1), preferred_element_type=F32
                )
            for a in range(16):
                first = ROWS * (4 + a // 4) + 4 * c + a % 4
                put(work, WORK, first, 16, 4 * ROWS, total[16 * a : 16 * a + 16])
        for j in range(0, N, 8):
            block = take(work, WORK, (4 + j) * ROWS, 8 * ROWS).astype(BF16)
            send_y[g, pl.ds(j, 8)] = block.reshape(8, ROWS, B)
        recv_y[OWN * me + g] = send_y[g, me]
        back(g)

    for g in range(OWN):
        convolve(g)

    for g in range(OWN):
        of_slabs(recv_y, N - 1, sy.at[g], ry.at[g]).wait_recv()
    squares = jnp.zeros((8, B), F32)
    for j in range(PAIRS):
        at = pl.ds(j * ROWS, ROWS)
        gain = skip_t[at, :]
        mixed = take(og_t, T, j * ROWS, ROWS) * (
            recv_y[j].astype(F32)
            + jnp.concatenate([gain, gain], axis=1) * send_x[j].astype(F32)
        )
        put(stage, T, j * ROWS, ROWS, 1, mixed)
        squares += mixed * mixed
    part[0:4, :] = squares[0:4] + squares[4:8]
    part[4:8, :] = jnp.zeros((4, B), F32)
    copies = []
    for k in range(1, 4):
        copy = pltpu.make_async_remote_copy(
            part, recv_p.at[k - 1], sp.at[k - 1], rp.at[k - 1],
            device_id={"mp": (mp + k) % 4}, device_id_type=MESH,
        )
        copy.start()
        copies.append(copy)
    for q in range(4):
        turned[pl.ds(q * B, B), :] = take(stage, T, q, CH, 4).T
    of_slabs(send_t, OWN * (N - 1), st, rt).wait_send()
    for g in range(OWN):
        of_slabs(send_x, N - 1, sx.at[g], rx.at[g]).wait_send()
        of_slabs(send_y.at[g], N - 1, sy.at[g], ry.at[g]).wait_send()
    power = part[0:4, :]
    for copy in copies:
        copy.wait_recv()
    power = power + recv_p[0][0:4] + recv_p[1][0:4] + recv_p[2][0:4]
    scale = 1.0 / jnp.sqrt(power / C + 1e-05)
    for q in range(4):
        column = jnp.broadcast_to(scale[q : q + 1], (128, B)).T
        column = jnp.concatenate([column, column], axis=1)
        out[pl.ds(q * B, B), :] = (turned[pl.ds(q * B, B), :] * column).astype(BF16)
    for copy in copies:
        copy.wait_send()


def local(gate_in, value_in, out_gate, filter_taps, skip_gain):
    arrays = (gate_in, value_in, out_gate, filter_taps, skip_gain.reshape(1, CH))
    vmem = pl.BlockSpec(memory_space=pltpu.VMEM)
    dma = pltpu.SemaphoreType.DMA
    return pl.pallas_call(
        kernel,
        out_shape=jax.ShapeDtypeStruct((T, CH), BF16),
        in_specs=[pl.BlockSpec(memory_space=pltpu.HBM)] * 5,
        out_specs=vmem,
        scratch_shapes=[
            pltpu.VMEM((T, CH), BF16),
            pltpu.VMEM((T, CH), BF16),
            pltpu.VMEM((T, CH), BF16),
            pltpu.VMEM((TAPS, CH), BF16),
            pltpu.VMEM((1, CH), F32),
            pltpu.VMEM((PAIRS, ROWS, B), BF16),
            pltpu.VMEM((PAIRS, 1, WIN), F32),
            pltpu.VMEM((OWN, N, ROWS, B), BF16),
            pltpu.VMEM((OWN * N, 1, WIN), F32),
            pltpu.VMEM((2 * T, 128), F32),
            pltpu.VMEM((2 * WORK, 128), F32),
            pltpu.VMEM((T, CH), F32),
            pltpu.VMEM((2 * T, 128), F32),
            pltpu.VMEM((T, 128), F32),
            pltpu.VMEM((PER * OWN, 40, WIN), F32),
            pltpu.VMEM((PER, 512, B), BF16),
            pltpu.VMEM((PER * OWN, BANDS * WIN, WIN), BF16),
            pltpu.VMEM((OWN, N, ROWS, B), BF16),
            pltpu.VMEM((PAIRS, ROWS, B), BF16),
            pltpu.VMEM((8, B), F32),
            pltpu.VMEM((3, 8, B), F32),
            dma((5,)), dma((OWN,)), dma((OWN,)), dma, dma, dma((OWN,)), dma((OWN,)), dma((3,)), dma((3,)),
        ],
        compiler_params=pltpu.CompilerParams(
            collective_id=0, has_side_effects=True, vmem_limit_bytes=40 * 2**20
        ),
    )(*[pltpu.with_memory_space_constraint(a, pltpu.HBM) for a in arrays])


def solution(mesh):
    return jax.shard_map(
        local,
        mesh=mesh,
        in_specs=(P("seq", "mp"), P("seq", "mp"), P("seq", "mp"), P("seq", "mp"), P("mp")),
        out_specs=P("seq", "mp"),
        check_vma=False,
    )
```

```python
import jax
import jax.numpy as jnp
from jax import lax
from jax.experimental import pallas as pl
from jax.experimental.pallas import tpu as pltpu
from jax.sharding import PartitionSpec as P

MESH = pl.DeviceIdType.MESH
F32 = jnp.float32
BF16 = jnp.bfloat16

C = 1024
B = 256
N = 64
T = 1024
CH = 256
TAPS = 64
WIN = 128
NWIN = 4096 // WIN
BANDS = 2 * 17 + 1
PER = 2
PAIRS = CH // PER
ROWS = 4 * PER
WORK = (N + 4) * ROWS
OWN = PAIRS // N


def place(me):
    return me // 32, me // 4 % 8, me % 4


ALONG = (4, 3, 5, 2, 6, 1, 7, 0)


def put(ref, size, first, count, stride, value):
    for h in range(2):
        ref[pl.ds(h * size + first, count, stride=stride), :] = value[:, 128 * h : 128 * h + 128]


def take(ref, size, first, count, stride=1):
    halves = [ref[pl.ds(h * size + first, count, stride=stride), :] for h in range(2)]
    return jnp.concatenate(halves, axis=1)


def kernel(
    gate_h, value_h, out_gate_h, taps_h, skip_h, out,
    gate, value, out_gate, taps, skip,
    send_x, send_t, recv_x, recv_t, stage, work, turned, og_t, skip_t, win, planes, bands, send_y, recv_y,
    part, recv_p, loaded, sx, rx, st, rt, sy, ry, sp, rp,
):
    me = lax.axis_index("seq")
    mp = lax.axis_index("mp")
    barrier = pltpu.get_barrier_semaphore()

    x, z, y = place(me)
    along = [(z + dz) % 8 * 4 for dz in ALONG]

    def others(visit):
        def column(r, last):
            dx, dy = (r + 1) % 8 // 4, (r + 1) % 4
            base = (x + dx) % 2 * 32 + (y + dy) % 4
            for plane in along[: 8 - last]:
                visit(base + plane)

        def each(r, carry):
            column(r, 0)
            return carry

        lax.fori_loop(0, 7, each, 0)
        column(7, 1)

    others(
        lambda to: pl.semaphore_signal(
            barrier, inc=1, device_id={"seq": to}, device_id_type=MESH
        )
    )
    for k in range(1, 4):
        pl.semaphore_signal(barrier, inc=1, device_id={"mp": (mp + k) % 4}, device_id_type=MESH)

    pairs = ((taps_h, taps), (gate_h, gate), (value_h, value), (out_gate_h, out_gate), (skip_h, skip))
    loads = [pltpu.make_async_copy(a, b, loaded.at[i]) for i, (a, b) in enumerate(pairs)]
    for load in loads:
        load.start()

    loads[0].wait()
    wide = jnp.concatenate([taps[...].astype(F32), jnp.zeros((128 - TAPS, CH), F32)], axis=0)
    stage[0:CH, :] = wide.T
    first, second = (stage[pl.ds(c, PAIRS, stride=PER), :] for c in range(PER))
    both = first + pltpu.roll(second, 64, 1)
    for j in range(N):
        send_t[j] = both[OWN * j : OWN * j + OWN].astype(BF16)

    loads[1].wait()
    loads[2].wait()
    for q in range(4):
        at = pl.ds(q * B, B)
        gated = (gate[at, :].astype(F32) * value[at, :].astype(F32)).astype(BF16)
        put(stage, T, q, CH, 4, gated.astype(F32).T)
    for j in range(0, N, 8):
        block = take(stage, T, j * 16, 128).astype(BF16)
        send_x[pl.ds(2 * j, 16)] = block.reshape(16, ROWS, B)
    pl.semaphore_wait(barrier, N - 1 + 3)

    def send(src, dst, ssem, rsem, to):
        pltpu.make_async_remote_copy(
            src, dst, ssem, rsem, device_id={"seq": to}, device_id_type=MESH
        ).start()

    def forth_taps(to):
        send(send_t.at[to], recv_t.at[me], st, rt, to)

    def forth(g):
        others(
            lambda to: send(
                send_x.at[OWN * to + g], recv_x.at[g, me], sx.at[g], rx.at[g], to
            )
        )

    def back(g):
        for half in range(2):
            half_planes = [(z + k) % 4 * 4 + 16 * half for k in range(4)]

            def go(to):
                send(send_y.at[g, to], recv_y.at[OWN * me + g], sy.at[g], ry.at[g], to)

            def column(r, first, half_planes=half_planes, go=go):
                dx, dy = (r + 1) % 8 // 4, (r + 1) % 4
                base = (x + dx) % 2 * 32 + (y + dy) % 4
                for plane in half_planes[first:]:
                    go(base + plane)

            def each(r, carry, column=column):
                column(r, 0)
                return carry

            lax.fori_loop(0, 7, each, 0)
            column(7, 1)

            @pl.when(z // 4 != half)
            def _(go=go, plane=half_planes[0]):
                go(x * 32 + y + plane)

    def of_slabs(ref, n, ssem, rsem):
        return pltpu.make_async_remote_copy(
            ref.at[pl.ds(0, n)], ref.at[pl.ds(0, n)], ssem, rsem,
            device_id={"seq": (me + 1) % N}, device_id_type=MESH,
        )

    others(forth_taps)
    for g in range(OWN):
        forth(g)
    recv_t[me] = send_t[me]
    for g in range(OWN):
        recv_x[g, me] = send_x[OWN * me + g]

    loads[3].wait()
    loads[4].wait()
    for q in range(4):
        put(og_t, T, q, CH, 4, out_gate[pl.ds(q * B, B), :].astype(F32).T)
        skip_t[pl.ds(q, CH, stride=4), :] = jnp.broadcast_to(skip[...], (128, CH)).T

    lane = lax.broadcasted_iota(jnp.int32, (OWN, WIN), 1)
    win[...] = jnp.zeros_like(win)
    of_slabs(recv_t, N - 1, st, rt).wait_recv()
    for j in range(NWIN):
        even, odd = recv_t[2 * j].astype(F32), recv_t[2 * j + 1].astype(F32)
        one = jnp.where(lane < 64, even, pltpu.roll(odd, 64, 1))
        two = jnp.where(lane < 64, pltpu.roll(even, 64, 1), odd)
        for g in range(OWN):
            win[2 * g, pl.ds(j + 1, 1), :] = one[g : g + 1]
            win[2 * g + 1, pl.ds(j + 1, 1), :] = two[g : g + 1]
    after = lax.broadcasted_iota(jnp.int32, (WIN, WIN), 1) >= lax.broadcasted_iota(
        jnp.int32, (WIN, WIN), 0
    )

    def banded(c, carry):
        before = jnp.zeros((WIN, WIN), F32)
        bands[c, pl.ds((BANDS - 1) * WIN, WIN), :] = before.astype(BF16)
        for v in range(NWIN + 1):
            row = jnp.broadcast_to(win[c, v + 1 : v + 2, :], (WIN, WIN))
            rolled = pltpu.roll(row, 0, 1, stride=1, stride_axis=0)
            at = pl.ds((BANDS - 2 - v) * WIN, WIN)
            bands[c, at, :] = jnp.where(after, rolled, before).astype(BF16)
            before = rolled
        bands[c, pl.ds(0, WIN), :] = jnp.zeros((WIN, WIN), BF16)
        return carry

    lax.fori_loop(0, PER * OWN, banded, 0)

    put(work, WORK, 0, 4 * ROWS, 1, jnp.zeros((4 * ROWS, B), F32))

    def convolve(g):
        of_slabs(recv_x.at[g], N - 1, sx.at[g], rx.at[g]).wait_recv()
        for j in range(0, N, 8):
            block = recv_x[g, pl.ds(j, 8)].reshape(8 * ROWS, B).astype(F32)
            put(work, WORK, (4 + j) * ROWS, 8 * ROWS, 1, block)
        for c in range(PER):
            for a in range(16):
                first = ROWS * (a // 4) + 4 * c + a % 4
                for late in range(2):
                    rows = take(work, WORK, first + 4 * ROWS * late, 16, 4 * ROWS)
                    planes[c, pl.ds(256 * late + 16 * a, 16), :] = rows.astype(BF16)
        for c in range(PER):
            total = jnp.zeros((256, B), F32)
            for d in range(17):
                left = planes[c, pl.ds((16 - d) * 16, 256), :]
                low = bands[PER * g + c, pl.ds((33 - 2 * d) * WIN, 2 * WIN), :]
                high = bands[PER * g + c, pl.ds((32 - 2 * d) * WIN, 2 * WIN), :]
                total += jnp.dot(
                    left, jnp.concatenate([low, high], axis=1), preferred_element_type=F32
                )
            for a in range(16):
                first = ROWS * (4 + a // 4) + 4 * c + a % 4
                put(work, WORK, first, 16, 4 * ROWS, total[16 * a : 16 * a + 16])
        for j in range(0, N, 8):
            block = take(work, WORK, (4 + j) * ROWS, 8 * ROWS).astype(BF16)
            send_y[g, pl.ds(j, 8)] = block.reshape(8, ROWS, B)
        recv_y[OWN * me + g] = send_y[g, me]
        back(g)

    for g in range(OWN):
        convolve(g)

    for g in range(OWN):
        of_slabs(recv_y, N - 1, sy.at[g], ry.at[g]).wait_recv()
    squares = jnp.zeros((8, B), F32)
    for j in range(PAIRS):
        at = pl.ds(j * ROWS, ROWS)
        gain = skip_t[at, :]
        mixed = take(og_t, T, j * ROWS, ROWS) * (
            recv_y[j].astype(F32)
            + jnp.concatenate([gain, gain], axis=1) * send_x[j].astype(F32)
        )
        put(stage, T, j * ROWS, ROWS, 1, mixed)
        squares += mixed * mixed
    part[0:4, :] = squares[0:4] + squares[4:8]
    part[4:8, :] = jnp.zeros((4, B), F32)
    copies = []
    for k in range(1, 4):
        copy = pltpu.make_async_remote_copy(
            part, recv_p.at[k - 1], sp.at[k - 1], rp.at[k - 1],
            device_id={"mp": (mp + k) % 4}, device_id_type=MESH,
        )
        copy.start()
        copies.append(copy)
    for q in range(4):
        turned[pl.ds(q * B, B), :] = take(stage, T, q, CH, 4).T
    of_slabs(send_t, N - 1, st, rt).wait_send()
    for g in range(OWN):
        of_slabs(send_x, N - 1, sx.at[g], rx.at[g]).wait_send()
        of_slabs(send_y.at[g], N - 1, sy.at[g], ry.at[g]).wait_send()
    power = part[0:4, :]
    for copy in copies:
        copy.wait_recv()
    power = power + recv_p[0][0:4] + recv_p[1][0:4] + recv_p[2][0:4]
    scale = 1.0 / jnp.sqrt(power / C + 1e-05)
    for q in range(4):
        column = jnp.broadcast_to(scale[q : q + 1], (128, B)).T
        column = jnp.concatenate([column, column], axis=1)
        out[pl.ds(q * B, B), :] = (turned[pl.ds(q * B, B), :] * column).astype(BF16)
    for copy in copies:
        copy.wait_send()


def local(gate_in, value_in, out_gate, filter_taps, skip_gain):
    arrays = (gate_in, value_in, out_gate, filter_taps, skip_gain.reshape(1, CH))
    vmem = pl.BlockSpec(memory_space=pltpu.VMEM)
    dma = pltpu.SemaphoreType.DMA
    return pl.pallas_call(
        kernel,
        out_shape=jax.ShapeDtypeStruct((T, CH), BF16),
        in_specs=[pl.BlockSpec(memory_space=pltpu.HBM)] * 5,
        out_specs=vmem,
        scratch_shapes=[
            pltpu.VMEM((T, CH), BF16),
            pltpu.VMEM((T, CH), BF16),
            pltpu.VMEM((T, CH), BF16),
            pltpu.VMEM((TAPS, CH), BF16),
            pltpu.VMEM((1, CH), F32),
            pltpu.VMEM((PAIRS, ROWS, B), BF16),
            pltpu.VMEM((N, OWN, WIN), BF16),
            pltpu.VMEM((OWN, N, ROWS, B), BF16),
            pltpu.VMEM((N, OWN, WIN), BF16),
            pltpu.VMEM((2 * T, 128), F32),
            pltpu.VMEM((2 * WORK, 128), F32),
            pltpu.VMEM((T, CH), F32),
            pltpu.VMEM((2 * T, 128), F32),
            pltpu.VMEM((T, 128), F32),
            pltpu.VMEM((PER * OWN, 40, WIN), F32),
            pltpu.VMEM((PER, 512, B), BF16),
            pltpu.VMEM((PER * OWN, BANDS * WIN, WIN), BF16),
            pltpu.VMEM((OWN, N, ROWS, B), BF16),
            pltpu.VMEM((PAIRS, ROWS, B), BF16),
            pltpu.VMEM((8, B), F32),
            pltpu.VMEM((3, 8, B), F32),
            dma((5,)), dma((OWN,)), dma((OWN,)), dma, dma, dma((OWN,)), dma((OWN,)), dma((3,)), dma((3,)),
        ],
        compiler_params=pltpu.CompilerParams(
            collective_id=0, has_side_effects=True, vmem_limit_bytes=40 * 2**20
        ),
    )(*[pltpu.with_memory_space_constraint(a, pltpu.HBM) for a in arrays])


def solution(mesh):
    return jax.shard_map(
        local,
        mesh=mesh,
        in_specs=(P("seq", "mp"), P("seq", "mp"), P("seq", "mp"), P("seq", "mp"), P("mp")),
        out_specs=P("seq", "mp"),
        check_vma=False,
    )
```

```python
import jax
import jax.numpy as jnp
from jax import lax
from jax.experimental import pallas as pl
from jax.experimental.pallas import tpu as pltpu
from jax.sharding import PartitionSpec as P

MESH = pl.DeviceIdType.MESH
F32 = jnp.float32
BF16 = jnp.bfloat16

C = 1024
B = 256
N = 64
T = 1024
CH = 256
TAPS = 64
WIN = 128
NWIN = 4096 // WIN
BANDS = 2 * 17 + 1
ROWS = 4
WORK = (N + 4) * ROWS
OWN = CH // N


def place(me):
    return me // 32, me // 4 % 8, me % 4


ALONG = (4, 3, 5, 2, 6, 1, 7, 0)


def put(ref, size, first, count, stride, value):
    for h in range(2):
        ref[pl.ds(h * size + first, count, stride=stride), :] = value[:, 128 * h : 128 * h + 128]


def take(ref, size, first, count, stride=1):
    halves = [ref[pl.ds(h * size + first, count, stride=stride), :] for h in range(2)]
    return jnp.concatenate(halves, axis=1)


def kernel(
    gate_h, value_h, out_gate_h, taps_h, skip_h, out,
    gate, value, out_gate, taps, skip,
    send_x, send_t, recv_x, recv_t, stage, work, turned, og_t, skip_t, win, planes, bands, send_y, recv_y,
    part, recv_p, loaded, sx, rx, st, rt, sy, ry, sp, rp,
):
    me = lax.axis_index("seq")
    mp = lax.axis_index("mp")
    barrier = pltpu.get_barrier_semaphore()

    x, z, y = place(me)
    along = [(z + dz) % 8 * 4 for dz in ALONG]

    def others(visit):
        def column(r, last):
            dx, dy = (r + 1) % 8 // 4, (r + 1) % 4
            base = (x + dx) % 2 * 32 + (y + dy) % 4
            for plane in along[: 8 - last]:
                visit(base + plane)

        def each(r, carry):
            column(r, 0)
            return carry

        lax.fori_loop(0, 7, each, 0)
        column(7, 1)

    others(
        lambda to: pl.semaphore_signal(
            barrier, inc=1, device_id={"seq": to}, device_id_type=MESH
        )
    )
    for k in range(1, 4):
        pl.semaphore_signal(barrier, inc=1, device_id={"mp": (mp + k) % 4}, device_id_type=MESH)

    pairs = ((taps_h, taps), (gate_h, gate), (value_h, value), (out_gate_h, out_gate), (skip_h, skip))
    loads = [pltpu.make_async_copy(a, b, loaded.at[i]) for i, (a, b) in enumerate(pairs)]
    for load in loads:
        load.start()

    loads[0].wait()
    wide = jnp.concatenate([taps[...].astype(F32), jnp.zeros((128 - TAPS, CH), F32)], axis=0)
    stage[0:CH, :] = wide.T
    first, second = (stage[pl.ds(c, CH // 2, stride=2), :] for c in range(2))
    both = first + pltpu.roll(second, 64, 1)
    for j in range(N):
        send_t[j] = both[2 * j : 2 * j + 2].astype(BF16)

    loads[1].wait()
    loads[2].wait()
    for q in range(4):
        at = pl.ds(q * B, B)
        gated = (gate[at, :].astype(F32) * value[at, :].astype(F32)).astype(BF16)
        put(stage, T, q, CH, 4, gated.astype(F32).T)
    for j in range(0, N, 8):
        block = take(stage, T, j * 16, 128).astype(BF16)
        send_x[pl.ds(OWN * j, 8 * OWN)] = block.reshape(8 * OWN, ROWS, B)
    pl.semaphore_wait(barrier, N - 1 + 3)

    def send(src, dst, ssem, rsem, to):
        pltpu.make_async_remote_copy(
            src, dst, ssem, rsem, device_id={"seq": to}, device_id_type=MESH
        ).start()

    def forth_taps(to):
        send(send_t.at[to], recv_t.at[me], st, rt, to)

    def by_halves(visit, order):
        for half in order:
            half_planes = [(z + k) % 4 * 4 + 16 * half for k in range(4)]

            def column(r, first, half_planes=half_planes):
                dx, dy = (r + 1) % 8 // 4, (r + 1) % 4
                base = (x + dx) % 2 * 32 + (y + dy) % 4
                for plane in half_planes[first:]:
                    visit(base + plane)

            def each(r, carry, column=column):
                column(r, 0)
                return carry

            lax.fori_loop(0, 7, each, 0)
            column(7, 1)

            @pl.when(z // 4 != half)
            def _(plane=half_planes[0]):
                visit(x * 32 + y + plane)

    def forth(g):
        others(
            lambda to: send(
                send_x.at[OWN * to + g], recv_x.at[g, me], sx.at[g], rx.at[g], to
            )
        )

    def back(g, halves):
        by_halves(
            lambda to: send(
                send_y.at[g, to], recv_y.at[OWN * me + g], sy.at[g], ry.at[g], to
            ),
            halves,
        )

    def of_slabs(ref, n, ssem, rsem):
        return pltpu.make_async_remote_copy(
            ref.at[pl.ds(0, n)], ref.at[pl.ds(0, n)], ssem, rsem,
            device_id={"seq": (me + 1) % N}, device_id_type=MESH,
        )

    others(forth_taps)
    for g in range(OWN):
        forth(g)
    recv_t[me] = send_t[me]
    for g in range(OWN):
        recv_x[g, me] = send_x[OWN * me + g]

    loads[3].wait()
    loads[4].wait()
    for q in range(4):
        put(og_t, T, q, CH, 4, out_gate[pl.ds(q * B, B), :].astype(F32).T)
        skip_t[pl.ds(q, CH, stride=4), :] = jnp.broadcast_to(skip[...], (128, CH)).T

    lane = lax.broadcasted_iota(jnp.int32, (2, WIN), 1)
    win[...] = jnp.zeros_like(win)
    of_slabs(recv_t, N - 1, st, rt).wait_recv()
    for j in range(NWIN):
        even, odd = recv_t[2 * j].astype(F32), recv_t[2 * j + 1].astype(F32)
        one = jnp.where(lane < 64, even, pltpu.roll(odd, 64, 1))
        two = jnp.where(lane < 64, pltpu.roll(even, 64, 1), odd)
        for g in range(2):
            win[2 * g, pl.ds(j + 1, 1), :] = one[g : g + 1]
            win[2 * g + 1, pl.ds(j + 1, 1), :] = two[g : g + 1]
    after = lax.broadcasted_iota(jnp.int32, (WIN, WIN), 1) >= lax.broadcasted_iota(
        jnp.int32, (WIN, WIN), 0
    )

    def banded(c, carry):
        before = jnp.zeros((WIN, WIN), F32)
        bands[c, pl.ds((BANDS - 1) * WIN, WIN), :] = before.astype(BF16)
        for v in range(NWIN + 1):
            row = jnp.broadcast_to(win[c, v + 1 : v + 2, :], (WIN, WIN))
            rolled = pltpu.roll(row, 0, 1, stride=1, stride_axis=0)
            at = pl.ds((BANDS - 2 - v) * WIN, WIN)
            bands[c, at, :] = jnp.where(after, rolled, before).astype(BF16)
            before = rolled
        bands[c, pl.ds(0, WIN), :] = jnp.zeros((WIN, WIN), BF16)
        return carry

    lax.fori_loop(0, OWN, banded, 0)

    put(work, WORK, 0, 4 * ROWS, 1, jnp.zeros((4 * ROWS, B), F32))

    def convolve(g):
        of_slabs(recv_x.at[g], N - 1, sx.at[g], rx.at[g]).wait_recv()
        for j in range(0, N, 8):
            block = recv_x[g, pl.ds(j, 8)].reshape(8 * ROWS, B).astype(F32)
            put(work, WORK, (4 + j) * ROWS, 8 * ROWS, 1, block)
        for a in range(16):
            first = ROWS * (a // 4) + a % 4
            for late in range(2):
                rows = take(work, WORK, first + 4 * ROWS * late, 16, 4 * ROWS)
                planes[pl.ds(256 * late + 16 * a, 16), :] = rows.astype(BF16)
        total = jnp.zeros((256, B), F32)
        for d in range(17):
            left = planes[pl.ds((16 - d) * 16, 256), :]
            low = bands[g, pl.ds((33 - 2 * d) * WIN, 2 * WIN), :]
            high = bands[g, pl.ds((32 - 2 * d) * WIN, 2 * WIN), :]
            total += jnp.dot(left, jnp.concatenate([low, high], axis=1), preferred_element_type=F32)
        for a in range(16):
            first = ROWS * (4 + a // 4) + a % 4
            put(work, WORK, first, 16, 4 * ROWS, total[16 * a : 16 * a + 16])
        for j in range(0, N, 8):
            block = take(work, WORK, (4 + j) * ROWS, 8 * ROWS).astype(BF16)
            send_y[g, pl.ds(j, 8)] = block.reshape(8, ROWS, B)
        recv_y[OWN * me + g] = send_y[g, me]
        back(g, (0, 1) if g < OWN - 2 else (0,))

    for g in range(OWN):
        convolve(g)
    for g in range(OWN - 2, OWN):
        back(g, (1,))

    squares = jnp.zeros((8, B), F32)
    for g in range(OWN):
        of_slabs(recv_y, N - 1, sy.at[g], ry.at[g]).wait_recv()
    for j in range(0, CH, 2):
        at = pl.ds(j * ROWS, 2 * ROWS)
        gain = skip_t[at, :]
        conv = recv_y[pl.ds(j, 2)].reshape(2 * ROWS, B).astype(F32)
        gated = send_x[pl.ds(j, 2)].reshape(2 * ROWS, B).astype(F32)
        mixed = take(og_t, T, j * ROWS, 2 * ROWS) * (
            conv + jnp.concatenate([gain, gain], axis=1) * gated
        )
        put(stage, T, j * ROWS, 2 * ROWS, 1, mixed)
        squares += mixed * mixed
    part[...] = squares[0:4] + squares[4:8]
    copies = []
    for k in range(1, 4):
        copy = pltpu.make_async_remote_copy(
            part, recv_p.at[k - 1], sp.at[k - 1], rp.at[k - 1],
            device_id={"mp": (mp + k) % 4}, device_id_type=MESH,
        )
        copy.start()
        copies.append(copy)
    for q in range(4):
        turned[pl.ds(q * B, B), :] = take(stage, T, q, CH, 4).T
    of_slabs(send_t, N - 1, st, rt).wait_send()
    for g in range(OWN):
        of_slabs(send_x, N - 1, sx.at[g], rx.at[g]).wait_send()
        of_slabs(send_y.at[g], N - 1, sy.at[g], ry.at[g]).wait_send()
    power = part[...]
    for copy in copies:
        copy.wait_recv()
    power = power + recv_p[0] + recv_p[1] + recv_p[2]
    scale = 1.0 / jnp.sqrt(power / C + 1e-05)
    for q in range(4):
        column = jnp.broadcast_to(scale[q : q + 1], (128, B)).T
        column = jnp.concatenate([column, column], axis=1)
        out[pl.ds(q * B, B), :] = (turned[pl.ds(q * B, B), :] * column).astype(BF16)
    for copy in copies:
        copy.wait_send()


def local(gate_in, value_in, out_gate, filter_taps, skip_gain):
    arrays = (gate_in, value_in, out_gate, filter_taps, skip_gain.reshape(1, CH))
    vmem = pl.BlockSpec(memory_space=pltpu.VMEM)
    dma = pltpu.SemaphoreType.DMA
    return pl.pallas_call(
        kernel,
        out_shape=jax.ShapeDtypeStruct((T, CH), BF16),
        in_specs=[pl.BlockSpec(memory_space=pltpu.HBM)] * 5,
        out_specs=vmem,
        scratch_shapes=[
            pltpu.VMEM((T, CH), BF16),
            pltpu.VMEM((T, CH), BF16),
            pltpu.VMEM((T, CH), BF16),
            pltpu.VMEM((TAPS, CH), BF16),
            pltpu.VMEM((1, CH), F32),
            pltpu.VMEM((CH, ROWS, B), BF16),
            pltpu.VMEM((N, 2, WIN), BF16),
            pltpu.VMEM((OWN, N, ROWS, B), BF16),
            pltpu.VMEM((N, 2, WIN), BF16),
            pltpu.VMEM((2 * T, 128), F32),
            pltpu.VMEM((2 * WORK, 128), F32),
            pltpu.VMEM((T, CH), F32),
            pltpu.VMEM((2 * T, 128), F32),
            pltpu.VMEM((T, 128), F32),
            pltpu.VMEM((OWN, 40, WIN), F32),
            pltpu.VMEM((512, B), BF16),
            pltpu.VMEM((OWN, BANDS * WIN, WIN), BF16),
            pltpu.VMEM((OWN, N, ROWS, B), BF16),
            pltpu.VMEM((CH, ROWS, B), BF16),
            pltpu.VMEM((4, B), F32),
            pltpu.VMEM((3, 4, B), F32),
            dma((5,)), dma((OWN,)), dma((OWN,)), dma, dma, dma((OWN,)), dma((OWN,)), dma((3,)), dma((3,)),
        ],
        compiler_params=pltpu.CompilerParams(
            collective_id=0, has_side_effects=True, vmem_limit_bytes=40 * 2**20
        ),
    )(*[pltpu.with_memory_space_constraint(a, pltpu.HBM) for a in arrays])


def solution(mesh):
    return jax.shard_map(
        local,
        mesh=mesh,
        in_specs=(P("seq", "mp"), P("seq", "mp"), P("seq", "mp"), P("seq", "mp"), P("mp")),
        out_specs=P("seq", "mp"),
        check_vma=False,
    )
```

```python
import jax
import jax.numpy as jnp
from jax import lax
from jax.experimental import pallas as pl
from jax.experimental.pallas import tpu as pltpu
from jax.sharding import PartitionSpec as P

MESH = pl.DeviceIdType.MESH
F32 = jnp.float32
BF16 = jnp.bfloat16

C = 1024
B = 256
N = 64
T = 1024
CH = 256
TAPS = 64
WIN = 128
NWIN = 4096 // WIN
BANDS = 2 * 17 + 1
ROWS = 4
WORK = (N + 4) * ROWS
OWN = CH // N


def place(me):
    return me // 32, me // 4 % 8, me % 4


ALONG = (4, 3, 5, 2, 6, 1, 7, 0)


def put(ref, size, first, count, stride, value):
    for h in range(2):
        ref[pl.ds(h * size + first, count, stride=stride), :] = value[:, 128 * h : 128 * h + 128]


def take(ref, size, first, count, stride=1):
    halves = [ref[pl.ds(h * size + first, count, stride=stride), :] for h in range(2)]
    return jnp.concatenate(halves, axis=1)


def kernel(
    gate_h, value_h, out_gate_h, taps_h, skip_h, out,
    gate, value, out_gate, taps, skip,
    send_x, send_t, recv_x, recv_t, stage, work, turned, og_t, skip_t, win, planes, bands, send_y, recv_y,
    part, recv_p, loaded, sx, rx, st, rt, sy, ry, sp, rp,
):
    me = lax.axis_index("seq")
    mp = lax.axis_index("mp")
    barrier = pltpu.get_barrier_semaphore()

    x, z, y = place(me)
    along = [(z + dz) % 8 * 4 for dz in ALONG]

    def others(visit):
        def column(r, last):
            dx, dy = (r + 1) % 8 // 4, (r + 1) % 4
            base = (x + dx) % 2 * 32 + (y + dy) % 4
            for plane in along[: 8 - last]:
                visit(base + plane)

        def each(r, carry):
            column(r, 0)
            return carry

        lax.fori_loop(0, 7, each, 0)
        column(7, 1)

    others(
        lambda to: pl.semaphore_signal(
            barrier, inc=1, device_id={"seq": to}, device_id_type=MESH
        )
    )
    for k in range(1, 4):
        pl.semaphore_signal(barrier, inc=1, device_id={"mp": (mp + k) % 4}, device_id_type=MESH)

    pairs = ((taps_h, taps), (gate_h, gate), (value_h, value), (out_gate_h, out_gate), (skip_h, skip))
    loads = [pltpu.make_async_copy(a, b, loaded.at[i]) for i, (a, b) in enumerate(pairs)]
    for load in loads:
        load.start()

    loads[0].wait()
    wide = jnp.concatenate([taps[...].astype(F32), jnp.zeros((128 - TAPS, CH), F32)], axis=0)
    stage[0:CH, :] = wide.T
    first, second = (stage[pl.ds(c, CH // 2, stride=2), :] for c in range(2))
    both = first + pltpu.roll(second, 64, 1)
    for j in range(N):
        send_t[j] = both[2 * j : 2 * j + 2].astype(BF16)

    loads[1].wait()
    loads[2].wait()
    for q in range(4):
        at = pl.ds(q * B, B)
        gated = (gate[at, :].astype(F32) * value[at, :].astype(F32)).astype(BF16)
        put(stage, T, q, CH, 4, gated.astype(F32).T)
    for j in range(0, N, 8):
        block = take(stage, T, j * 16, 128).astype(BF16)
        send_x[pl.ds(OWN * j, 8 * OWN)] = block.reshape(8 * OWN, ROWS, B)
    pl.semaphore_wait(barrier, N - 1 + 3)

    def send(src, dst, ssem, rsem, to):
        pltpu.make_async_remote_copy(
            src, dst, ssem, rsem, device_id={"seq": to}, device_id_type=MESH
        ).start()

    def forth_taps(to):
        send(send_t.at[to], recv_t.at[me], st, rt, to)

    def by_halves(visit, order):
        for half in order:
            half_planes = [(z + k) % 4 * 4 + 16 * half for k in range(4)]

            def column(r, first, half_planes=half_planes):
                dx, dy = (r + 1) % 8 // 4, (r + 1) % 4
                base = (x + dx) % 2 * 32 + (y + dy) % 4
                for plane in half_planes[first:]:
                    visit(base + plane)

            def each(r, carry, column=column):
                column(r, 0)
                return carry

            lax.fori_loop(0, 7, each, 0)
            column(7, 1)

            @pl.when(z // 4 != half)
            def _(plane=half_planes[0]):
                visit(x * 32 + y + plane)

    def forth(g):
        others(
            lambda to: send(
                send_x.at[OWN * to + g], recv_x.at[g, me], sx.at[g], rx.at[g], to
            )
        )

    def back(g, halves):
        by_halves(
            lambda to: send(
                send_y.at[g, to], recv_y.at[OWN * me + g], sy.at[g], ry.at[g], to
            ),
            halves,
        )

    def of_slabs(ref, n, ssem, rsem):
        return pltpu.make_async_remote_copy(
            ref.at[pl.ds(0, n)], ref.at[pl.ds(0, n)], ssem, rsem,
            device_id={"seq": (me + 1) % N}, device_id_type=MESH,
        )

    others(forth_taps)
    for g in range(OWN):
        forth(g)
    recv_t[me] = send_t[me]
    for g in range(OWN):
        recv_x[g, me] = send_x[OWN * me + g]

    loads[3].wait()
    loads[4].wait()
    for q in range(4):
        put(og_t, T, q, CH, 4, out_gate[pl.ds(q * B, B), :].astype(F32).T)
        skip_t[pl.ds(q, CH, stride=4), :] = jnp.broadcast_to(skip[...], (128, CH)).T

    lane = lax.broadcasted_iota(jnp.int32, (2, WIN), 1)
    win[...] = jnp.zeros_like(win)
    of_slabs(recv_t, N - 1, st, rt).wait_recv()
    for j in range(NWIN):
        even, odd = recv_t[2 * j].astype(F32), recv_t[2 * j + 1].astype(F32)
        one = jnp.where(lane < 64, even, pltpu.roll(odd, 64, 1))
        two = jnp.where(lane < 64, pltpu.roll(even, 64, 1), odd)
        for g in range(2):
            win[2 * g, pl.ds(j + 1, 1), :] = one[g : g + 1]
            win[2 * g + 1, pl.ds(j + 1, 1), :] = two[g : g + 1]
    after = lax.broadcasted_iota(jnp.int32, (WIN, WIN), 1) >= lax.broadcasted_iota(
        jnp.int32, (WIN, WIN), 0
    )

    def banded(c, carry):
        before = jnp.zeros((WIN, WIN), F32)
        bands[c, pl.ds((BANDS - 1) * WIN, WIN), :] = before.astype(BF16)
        for v in range(NWIN + 1):
            row = jnp.broadcast_to(win[c, v + 1 : v + 2, :], (WIN, WIN))
            rolled = pltpu.roll(row, 0, 1, stride=1, stride_axis=0)
            at = pl.ds((BANDS - 2 - v) * WIN, WIN)
            bands[c, at, :] = jnp.where(after, rolled, before).astype(BF16)
            before = rolled
        bands[c, pl.ds(0, WIN), :] = jnp.zeros((WIN, WIN), BF16)
        return carry

    lax.fori_loop(0, OWN, banded, 0)

    put(work, WORK, 0, 4 * ROWS, 1, jnp.zeros((4 * ROWS, B), F32))

    def convolve(g):
        of_slabs(recv_x.at[g], N - 1, sx.at[g], rx.at[g]).wait_recv()
        for j in range(0, N, 8):
            block = recv_x[g, pl.ds(j, 8)].reshape(8 * ROWS, B).astype(F32)
            put(work, WORK, (4 + j) * ROWS, 8 * ROWS, 1, block)
        for a in range(16):
            first = ROWS * (a // 4) + a % 4
            for late in range(2):
                rows = take(work, WORK, first + 4 * ROWS * late, 16, 4 * ROWS)
                planes[pl.ds(256 * late + 16 * a, 16), :] = rows.astype(BF16)
        total = jnp.zeros((256, B), F32)
        for d in range(17):
            left = planes[pl.ds((16 - d) * 16, 256), :]
            low = bands[g, pl.ds((33 - 2 * d) * WIN, 2 * WIN), :]
            high = bands[g, pl.ds((32 - 2 * d) * WIN, 2 * WIN), :]
            total += jnp.dot(left, jnp.concatenate([low, high], axis=1), preferred_element_type=F32)
        for a in range(16):
            first = ROWS * (4 + a // 4) + a % 4
            put(work, WORK, first, 16, 4 * ROWS, total[16 * a : 16 * a + 16])
        for j in range(0, N, 8):
            block = take(work, WORK, (4 + j) * ROWS, 8 * ROWS).astype(BF16)
            send_y[g, pl.ds(j, 8)] = block.reshape(8, ROWS, B)
        recv_y[OWN * me + g] = send_y[g, me]
        back(g, (0, 1) if g < OWN - 2 else (0,))

    for g in range(OWN):
        convolve(g)
    for g in range(OWN - 2, OWN):
        back(g, (1,))

    squares = jnp.zeros((8, B), F32)
    for g in range(0, OWN, 2):
        for h in (g, g + 1):
            of_slabs(recv_y, N - 1, sy.at[h], ry.at[h]).wait_recv()
        for j in range(g, CH, OWN):
            at = pl.ds(j * ROWS, 2 * ROWS)
            gain = skip_t[at, :]
            conv = recv_y[pl.ds(j, 2)].reshape(2 * ROWS, B).astype(F32)
            gated = send_x[pl.ds(j, 2)].reshape(2 * ROWS, B).astype(F32)
            mixed = take(og_t, T, j * ROWS, 2 * ROWS) * (
                conv + jnp.concatenate([gain, gain], axis=1) * gated
            )
            put(stage, T, j * ROWS, 2 * ROWS, 1, mixed)
            squares += mixed * mixed
    part[...] = squares[0:4] + squares[4:8]
    copies = []
    for k in range(1, 4):
        copy = pltpu.make_async_remote_copy(
            part, recv_p.at[k - 1], sp.at[k - 1], rp.at[k - 1],
            device_id={"mp": (mp + k) % 4}, device_id_type=MESH,
        )
        copy.start()
        copies.append(copy)
    for q in range(4):
        turned[pl.ds(q * B, B), :] = take(stage, T, q, CH, 4).T
    of_slabs(send_t, N - 1, st, rt).wait_send()
    for g in range(OWN):
        of_slabs(send_x, N - 1, sx.at[g], rx.at[g]).wait_send()
        of_slabs(send_y.at[g], N - 1, sy.at[g], ry.at[g]).wait_send()
    power = part[...]
    for copy in copies:
        copy.wait_recv()
    power = power + recv_p[0] + recv_p[1] + recv_p[2]
    scale = 1.0 / jnp.sqrt(power / C + 1e-05)
    for q in range(4):
        column = jnp.broadcast_to(scale[q : q + 1], (128, B)).T
        column = jnp.concatenate([column, column], axis=1)
        out[pl.ds(q * B, B), :] = (turned[pl.ds(q * B, B), :] * column).astype(BF16)
    for copy in copies:
        copy.wait_send()


def local(gate_in, value_in, out_gate, filter_taps, skip_gain):
    arrays = (gate_in, value_in, out_gate, filter_taps, skip_gain.reshape(1, CH))
    vmem = pl.BlockSpec(memory_space=pltpu.VMEM)
    dma = pltpu.SemaphoreType.DMA
    return pl.pallas_call(
        kernel,
        out_shape=jax.ShapeDtypeStruct((T, CH), BF16),
        in_specs=[pl.BlockSpec(memory_space=pltpu.HBM)] * 5,
        out_specs=vmem,
        scratch_shapes=[
            pltpu.VMEM((T, CH), BF16),
            pltpu.VMEM((T, CH), BF16),
            pltpu.VMEM((T, CH), BF16),
            pltpu.VMEM((TAPS, CH), BF16),
            pltpu.VMEM((1, CH), F32),
            pltpu.VMEM((CH, ROWS, B), BF16),
            pltpu.VMEM((N, 2, WIN), BF16),
            pltpu.VMEM((OWN, N, ROWS, B), BF16),
            pltpu.VMEM((N, 2, WIN), BF16),
            pltpu.VMEM((2 * T, 128), F32),
            pltpu.VMEM((2 * WORK, 128), F32),
            pltpu.VMEM((T, CH), F32),
            pltpu.VMEM((2 * T, 128), F32),
            pltpu.VMEM((T, 128), F32),
            pltpu.VMEM((OWN, 40, WIN), F32),
            pltpu.VMEM((512, B), BF16),
            pltpu.VMEM((OWN, BANDS * WIN, WIN), BF16),
            pltpu.VMEM((OWN, N, ROWS, B), BF16),
            pltpu.VMEM((CH, ROWS, B), BF16),
            pltpu.VMEM((4, B), F32),
            pltpu.VMEM((3, 4, B), F32),
            dma((5,)), dma((OWN,)), dma((OWN,)), dma, dma, dma((OWN,)), dma((OWN,)), dma((3,)), dma((3,)),
        ],
        compiler_params=pltpu.CompilerParams(
            collective_id=0, has_side_effects=True, vmem_limit_bytes=40 * 2**20
        ),
    )(*[pltpu.with_memory_space_constraint(a, pltpu.HBM) for a in arrays])


def solution(mesh):
    return jax.shard_map(
        local,
        mesh=mesh,
        in_specs=(P("seq", "mp"), P("seq", "mp"), P("seq", "mp"), P("seq", "mp"), P("mp")),
        out_specs=P("seq", "mp"),
        check_vma=False,
    )
```
